32 devices in a mesh: expert: 2 (over core), task: 4 (over y, x), shard: 4 (over z).
Axes of the slice: x: 2, y: 2, z: 4, core: 2. Of those that a mesh axis runs over, the one named last changes fastest.
Arguments:
- weights: bfloat16 [4, 2, 8192, 2048], P('task', None, ('expert', 'shard')), may hold values from -6 to 6
- fisher: bfloat16 [4, 2, 8192, 2048], P('task', None, ('expert', 'shard')), may hold values from 0.049804688 to 5
- base_weights: bfloat16 [2, 8192, 2048], P('expert', 'task', 'shard'), may hold values from -6 to 6
- tile_list: int32 [4, 2, 8, 4], P('task'), may hold values from 0 to 7, as said below
- tile_count: int32 [4, 2, 8], P('task'), may hold values from 0 to 4, as said below
Outputs:
- merged: bfloat16 [2, 8192, 2048], P('expert', 'task', 'shard')
The draws below stay inside these ranges and needn't reach their ends.
Inputs may be any that keep to these rules, and one draw needn't show every extreme that they name: `tile_list`: for each fine-fit, expert and row block the first tile_count entries are distinct tiles of the block, numbered 0 to 7, in ascending order; the remaining entries are 0. `tile_count`: 4 is reached, and for each fine-fit some expert has 4 in every row block.
All inputs are finite; a program needn't handle non-finite values.
Results may differ from the reference program's by a relative error of at most 0.006.
Values may be sent and summed in bfloat16 or wider, within the bound.
A program may use at most 128 MiB of HBM per device.

```python
import math
import jax
import jax.numpy as jnp
from jax import lax

ROWS = 8192
COLS = 2048
TILE = 128
EXPERTS = 2
TASKS = 4
BLOCKS = 8
TPB = 8
CAP = 4


def tile_plan(key):
    base_key = jax.random.fold_in(key, 7)
    key_count, key_full, key_order = jax.random.split(base_key, 3)
    counts = jax.random.randint(key_count, (TASKS, EXPERTS, BLOCKS), 0, CAP + 1)
    full_expert = jax.random.randint(key_full, (TASKS,), 0, EXPERTS)
    is_full = jnp.arange(EXPERTS)[None, :, None] == full_expert[:, None, None]
    counts = jnp.where(is_full, CAP, counts).astype(jnp.int32)
    scores = jax.random.randint(key_order, (TASKS, EXPERTS, BLOCKS, TPB), 0, 1 << 20)
    scores = scores * TPB + jnp.arange(TPB)[None, None, None, :]
    chosen = jnp.argsort(scores, axis=-1)[..., :CAP]
    slot_live = jnp.arange(CAP)[None, None, None, :] < counts[..., None]
    marked = jnp.sort(jnp.where(slot_live, chosen, TPB), axis=-1)
    listed = jnp.where(marked == TPB, 0, marked).astype(jnp.int32)
    return (listed, counts)


def draw_tile_list(key, part):
    return tile_plan(key)[0]


def draw_tile_count(key, part):
    return tile_plan(key)[1]


def shard_levels(stream_key, shape, cuts, smallest, high):
    loudness, own = 1.0, jax.random.fold_in(stream_key, 6)
    for axis_at, blocks in cuts:
        steps = jnp.exp(jax.random.uniform(jax.random.fold_in(own, axis_at), (blocks,), jnp.float32, smallest / len(cuts), high / len(cuts)))
        loudness = loudness * jnp.repeat(steps, shape[axis_at] // blocks).reshape([-1 if axis == axis_at else 1 for axis in range(len(shape))])
    return loudness


def noise(rng, shape, scale, limit, cuts=(), kind=jnp.bfloat16):
    result = jax.random.normal(rng, shape, jnp.float32) * scale
    if len(cuts) > 0:
        result = shard_levels(rng, shape, cuts, -0.22, 0.18) * result
    return jnp.clip(result, min=-limit, max=limit).astype(kind)


def setup_inputs(seed: int = 0) -> dict:
    splits = jax.random.split(jax.random.key(seed), 6)
    weights = noise(splits[0], (TASKS, EXPERTS, ROWS, COLS), 1.0, 6.0, ((0, 4), (2, 8)))
    fisher = jnp.clip(jnp.exp(math.log(5.0) - 4.609084 * jax.random.uniform(splits[1], (TASKS, EXPERTS, ROWS, COLS), jnp.float32) ** shard_levels(splits[1], (TASKS, EXPERTS, ROWS, COLS), ((0, 4), (2, 8)), -0.2, 0.2)), 0.049804688, 5.0).astype(jnp.bfloat16)
    base_weights = noise(splits[2], (EXPERTS, ROWS, COLS), 1.0, 6.0, ((0, 2), (1, 4), (2, 4)))
    tile_list = draw_tile_list(jax.random.fold_in(splits[5], 71), 0)
    tile_count = draw_tile_count(jax.random.fold_in(splits[5], 71), 0)
    return dict(weights=weights, fisher=fisher, base_weights=base_weights, tile_list=tile_list, tile_count=tile_count)


PRIOR_WEIGHT = 0.5


def reference(weights, fisher, base_weights, tile_list, tile_count):
    numerator = jnp.zeros((EXPERTS, ROWS, COLS), jnp.float32)
    denominator = jnp.zeros((EXPERTS, ROWS, COLS), jnp.float32)
    for task_index in range(TASKS):
        slot_live = jnp.arange(CAP, dtype=jnp.int32)[None, None, :] < tile_count[task_index][:, :, None]
        matches = (tile_list[task_index][:, :, :, None] == jnp.arange(TPB, dtype=jnp.int32)[None, None, None, :]) & slot_live[:, :, :, None]
        kept_tiles = jnp.any(matches, axis=2).reshape(EXPERTS, BLOCKS * TPB).astype(jnp.float32)
        row_mask = jnp.repeat(kept_tiles, TILE, axis=1)[:, :, None]
        fisher_now = fisher[task_index].astype(jnp.float32) * row_mask
        term = (fisher_now * weights[task_index].astype(jnp.float32)).astype(jnp.bfloat16)
        term = lax.optimization_barrier(term)
        share = fisher_now.astype(jnp.bfloat16)
        share = lax.optimization_barrier(share)
        numerator = numerator + term.astype(jnp.float32)
        denominator = denominator + share.astype(jnp.float32)
    merged = (numerator + PRIOR_WEIGHT * base_weights.astype(jnp.float32)) / (denominator + PRIOR_WEIGHT)
    return merged.astype(jnp.bfloat16)
```

```python
import functools

import jax
import jax.numpy as jnp
from jax import lax
from jax.experimental import pallas as pl
from jax.experimental.pallas import tpu as pltpu
from jax.sharding import PartitionSpec as P

TILE = 128
PRIOR_WEIGHT = 0.5
MESH = pl.DeviceIdType.MESH


def pack_body(ids, live, weights, fisher, packed):
    expert, slot = pl.program_id(0), pl.program_id(1)
    kept = live[expert * pl.num_programs(1) + slot].astype(jnp.float32)
    pieces, width = packed.shape[1], packed.shape[-1]
    for piece in range(pieces):
        lanes = pl.ds(piece * width, width)
        share = fisher[0, :, lanes].astype(jnp.float32) * kept
        term = share * weights[0, :, lanes].astype(jnp.float32)
        packed[0, piece, 0, 0] = term.astype(jnp.bfloat16)
        packed[0, piece, 1, 0] = share.astype(jnp.bfloat16)


def pack(ids, live, weights, fisher, pieces):
    experts, rows, columns = weights.shape
    cap = ids.shape[0] // experts
    width = columns // pieces
    tile = pl.BlockSpec(
        (1, TILE, columns), lambda e, k, ids, live: (e, ids[e * cap + k], 0)
    )
    return pl.pallas_call(
        pack_body,
        out_shape=jax.ShapeDtypeStruct(
            (experts, pieces, 2, cap, TILE, width), jnp.bfloat16
        ),
        grid_spec=pltpu.PrefetchScalarGridSpec(
            num_scalar_prefetch=2,
            grid=(experts, cap),
            in_specs=[tile, tile],
            out_specs=pl.BlockSpec(
                (1, pieces, 2, 1, TILE, width), lambda e, k, ids, live: (e, 0, 0, k, 0, 0)
            ),
        ),
        name="pack",
    )(ids, live, weights, fisher)


def exchange_body(sizes, packed, received, send_sem, recv_sem, own_sem):
    experts, tasks, shards = sizes
    blocks = experts * shards
    group = blocks // tasks
    expert, task, shard = (lax.axis_index(a) for a in ("expert", "task", "shard"))
    block = expert * shards + shard
    owner = block // group
    place = block % group
    is_own = owner == task
    order = [(de, ds) for ds in range(shards - 1, -1, -1) for de in range(experts)]

    def outgoing(de, ds):
        to_expert = lax.rem(expert + de, experts)
        to_shard = lax.rem(shard + ds, shards)
        return pltpu.make_async_remote_copy(
            src_ref=packed.at[to_expert, to_shard],
            dst_ref=received.at[task, place],
            send_sem=send_sem.at[de, ds],
            recv_sem=recv_sem.at[task, place],
            device_id=(to_expert, owner, to_shard),
            device_id_type=MESH,
        )

    own = pltpu.make_async_copy(
        packed.at[expert, shard], received.at[task, place], own_sem
    )
    for de, ds in order:
        if (de, ds) == (0, 0):
            pl.when(is_own)(own.start)
            pl.when(jnp.logical_not(is_own))(outgoing(de, ds).start)
        else:
            outgoing(de, ds).start()
    for from_task in range(tasks):
        for at in range(group):
            local = jnp.logical_and(is_own, jnp.logical_and(task == from_task, place == at))
            arriving = pltpu.make_async_remote_copy(
                src_ref=packed.at[0, 0],
                dst_ref=received.at[from_task, at],
                send_sem=send_sem.at[0, 0],
                recv_sem=recv_sem.at[from_task, at],
                device_id=(lax.rem(expert + 1, experts), task, shard),
                device_id_type=MESH,
            )
            pl.when(jnp.logical_not(local))(arriving.wait_recv)
    for de, ds in order:
        if (de, ds) == (0, 0):
            pl.when(is_own)(own.wait)
            pl.when(jnp.logical_not(is_own))(outgoing(de, ds).wait_send)
        else:
            outgoing(de, ds).wait_send()


def exchange(packed, sizes):
    experts, tasks, shards = sizes
    group = experts * shards // tasks
    return pl.pallas_call(
        functools.partial(exchange_body, sizes),
        out_shape=jax.ShapeDtypeStruct((tasks, group) + packed.shape[2:], packed.dtype),
        in_specs=[pl.BlockSpec(memory_space=pl.ANY)],
        out_specs=pl.BlockSpec(memory_space=pl.ANY),
        scratch_shapes=[
            pltpu.SemaphoreType.DMA((experts, shards)),
            pltpu.SemaphoreType.DMA((tasks, group)),
            pltpu.SemaphoreType.DMA,
        ],
        compiler_params=pltpu.CompilerParams(has_side_effects=True),
        name="exchange",
    )(packed)


def merge_body(tasks, slots, live, *refs):
    parts, base, merged = refs[:tasks], refs[tasks], refs[tasks + 1]
    at = pl.program_id(0) * pl.num_programs(1) + pl.program_id(1)
    count = pl.num_programs(0) * pl.num_programs(1)
    numerator = PRIOR_WEIGHT * base[...].astype(jnp.float32)
    denominator = jnp.full(base.shape, PRIOR_WEIGHT, jnp.float32)
    for task, part in enumerate(parts):
        kept = live[task * count + at].astype(jnp.float32)
        numerator += part[0, 0, 0, 0].astype(jnp.float32) * kept
        denominator += part[0, 0, 1, 0].astype(jnp.float32) * kept
    merged[...] = (numerator / denominator).astype(jnp.bfloat16)


def merge(slots, live, received, base):
    tasks, group, _, _, _, width = received.shape
    per_block = slots.shape[0] // (tasks * group)

    def part(task):
        return pl.BlockSpec(
            (1, 1, 2, 1, TILE, width),
            lambda g, j, slots, live: (
                task, g, 0, slots[(task * group + g) * per_block + j], 0, 0
            ),
        )

    rows = pl.BlockSpec((TILE, width), lambda g, j, slots, live: (g * per_block + j, 0))
    return pl.pallas_call(
        functools.partial(merge_body, tasks),
        out_shape=jax.ShapeDtypeStruct(base.shape, jnp.bfloat16),
        grid_spec=pltpu.PrefetchScalarGridSpec(
            num_scalar_prefetch=2,
            grid=(group, per_block),
            in_specs=[part(task) for task in range(tasks)] + [rows],
            out_specs=rows,
        ),
        name="merge",
    )(slots, live, *([received] * tasks), base)


def local(weights, fisher, base_weights, tile_list, tile_count):
    experts, tasks, shards = (lax.axis_size(a) for a in ("expert", "task", "shard"))
    expert, task, shard = (lax.axis_index(a) for a in ("expert", "task", "shard"))
    per_block = weights.shape[2] // TILE
    cap = tile_list.shape[-1]
    group = experts * shards // tasks
    block = expert * shards + shard
    slot_number = jnp.arange(cap, dtype=jnp.int32)

    own_list = lax.dynamic_index_in_dim(tile_list[0], block, 1, keepdims=False)
    own_count = lax.dynamic_index_in_dim(tile_count[0], block, 1, keepdims=False)
    own_live = (slot_number[None, :] < own_count[:, None]).astype(jnp.int32)
    packed = pack(own_list.reshape(-1), own_live.reshape(-1), weights[0], fisher[0], shards)

    marked = jnp.where(slot_number < tile_count[..., None], tile_list, per_block)
    plans = lax.all_gather(marked[0], "task")
    plans = lax.dynamic_index_in_dim(plans, expert, 1, keepdims=False)
    plans = lax.dynamic_slice_in_dim(plans, task * group, group, 1)
    hits = plans[..., None] == jnp.arange(per_block, dtype=jnp.int32)
    slots = jnp.sum(hits * slot_number[:, None], axis=2).astype(jnp.int32)
    live = jnp.any(hits, axis=2).astype(jnp.int32)

    received = exchange(packed, (experts, tasks, shards))
    return merge(slots.reshape(-1), live.reshape(-1), received, base_weights[0])[None]


def solution(mesh):
    in_specs = (
        P("task", None, ("expert", "shard"), None),
        P("task", None, ("expert", "shard"), None),
        P("expert", "task", "shard"),
        P("task", None, None, None),
        P("task", None, None),
    )
    out_specs = P("expert", "task", "shard")
    return jax.shard_map(local, mesh=mesh, in_specs=in_specs, out_specs=out_specs, check_vma=False)
```

```python
import functools

import jax
import jax.numpy as jnp
from jax import lax
from jax.experimental import pallas as pl
from jax.experimental.pallas import tpu as pltpu
from jax.sharding import PartitionSpec as P

TILE = 128
PRIOR_WEIGHT = 0.5
DIRECT = 32
MESH = pl.DeviceIdType.MESH


def pack_body(ids, live, weights, fisher, packed):
    expert, slot = pl.program_id(0), pl.program_id(1)
    kept = live[expert * pl.num_programs(1) + slot].astype(jnp.float32)
    pieces, width = packed.shape[1], packed.shape[-1]
    for piece in range(pieces):
        lanes = pl.ds(piece * width, width)
        share = fisher[0, :, lanes].astype(jnp.float32) * kept
        term = share * weights[0, :, lanes].astype(jnp.float32)
        packed[0, piece, 0, 0] = term.astype(jnp.bfloat16)
        packed[0, piece, 1, 0] = share.astype(jnp.bfloat16)


def pack(ids, live, weights, fisher, pieces):
    experts, rows, columns = weights.shape
    cap = ids.shape[0] // experts
    width = columns // pieces
    tile = pl.BlockSpec(
        (1, TILE, columns), lambda e, k, ids, live: (e, ids[e * cap + k], 0)
    )
    return pl.pallas_call(
        pack_body,
        out_shape=jax.ShapeDtypeStruct(
            (experts, pieces, 2, cap, TILE, width), jnp.bfloat16
        ),
        grid_spec=pltpu.PrefetchScalarGridSpec(
            num_scalar_prefetch=2,
            grid=(experts, cap),
            in_specs=[tile, tile],
            out_specs=pl.BlockSpec(
                (1, pieces, 2, 1, TILE, width), lambda e, k, ids, live: (e, 0, 0, k, 0, 0)
            ),
        ),
        name="pack",
    )(ids, live, weights, fisher)


def exchange_body(sizes, packed, received, send_sem, recv_sem, own_sem):
    experts, tasks, shards = sizes
    blocks = experts * shards
    group = blocks // tasks
    expert, task, shard = (lax.axis_index(a) for a in ("expert", "task", "shard"))
    block = expert * shards + shard
    owner = block // group
    place = block % group
    is_own = owner == task
    order = [(de, ds) for ds in range(shards - 1, -1, -1) for de in range(experts)]

    def outgoing(de, ds):
        to_expert = lax.rem(expert + de, experts)
        to_shard = lax.rem(shard + ds, shards)
        return pltpu.make_async_remote_copy(
            src_ref=packed.at[to_expert, to_shard],
            dst_ref=received.at[task, place],
            send_sem=send_sem.at[de, ds],
            recv_sem=recv_sem.at[task, place],
            device_id=(to_expert, owner, to_shard),
            device_id_type=MESH,
        )

    own = pltpu.make_async_copy(
        packed.at[expert, shard], received.at[task, place], own_sem
    )
    for de, ds in order:
        if (de, ds) == (0, 0):
            pl.when(is_own)(own.start)
            pl.when(jnp.logical_not(is_own))(outgoing(de, ds).start)
        else:
            outgoing(de, ds).start()
    for from_task in range(tasks):
        for at in range(group):
            local = jnp.logical_and(is_own, jnp.logical_and(task == from_task, place == at))
            arriving = pltpu.make_async_remote_copy(
                src_ref=packed.at[0, 0],
                dst_ref=received.at[from_task, at],
                send_sem=send_sem.at[0, 0],
                recv_sem=recv_sem.at[from_task, at],
                device_id=(lax.rem(expert + 1, experts), task, shard),
                device_id_type=MESH,
            )
            pl.when(jnp.logical_not(local))(arriving.wait_recv)
    for de, ds in order:
        if (de, ds) == (0, 0):
            pl.when(is_own)(own.wait)
            pl.when(jnp.logical_not(is_own))(outgoing(de, ds).wait_send)
        else:
            outgoing(de, ds).wait_send()


def exchange(packed, sizes):
    experts, tasks, shards = sizes
    group = experts * shards // tasks
    return pl.pallas_call(
        functools.partial(exchange_body, sizes),
        out_shape=jax.ShapeDtypeStruct((tasks, group) + packed.shape[2:], packed.dtype),
        in_specs=[pl.BlockSpec(memory_space=pl.ANY)],
        out_specs=pl.BlockSpec(memory_space=pl.ANY),
        scratch_shapes=[
            pltpu.SemaphoreType.DMA((experts, shards)),
            pltpu.SemaphoreType.DMA((tasks, group)),
            pltpu.SemaphoreType.DMA,
        ],
        compiler_params=pltpu.CompilerParams(has_side_effects=True),
        name="exchange",
    )(packed)


def merge_body(tasks, slots, live, *refs):
    parts, base, merged = refs[:tasks], refs[tasks], refs[tasks + 1]
    at = pl.program_id(0) * pl.num_programs(1) + pl.program_id(1)
    count = pl.num_programs(0) * pl.num_programs(1)
    numerator = PRIOR_WEIGHT * base[...].astype(jnp.float32)
    denominator = jnp.full(base.shape, PRIOR_WEIGHT, jnp.float32)
    for task, part in enumerate(parts):
        kept = live[task * count + at].astype(jnp.float32)
        numerator += part[0, 0, 0, 0].astype(jnp.float32) * kept
        denominator += part[0, 0, 1, 0].astype(jnp.float32) * kept
    merged[...] = (numerator / denominator).astype(jnp.bfloat16)


def merge(slots, live, received, base):
    tasks, group, _, _, _, width = received.shape
    per_block = slots.shape[0] // (tasks * group)

    def part(task):
        return pl.BlockSpec(
            (1, 1, 2, 1, TILE, width),
            lambda g, j, slots, live: (
                task, g, 0, slots[(task * group + g) * per_block + j], 0, 0
            ),
        )

    rows = pl.BlockSpec((TILE, width), lambda g, j, slots, live: (g * per_block + j, 0))
    return pl.pallas_call(
        functools.partial(merge_body, tasks),
        out_shape=jax.ShapeDtypeStruct(base.shape, jnp.bfloat16),
        grid_spec=pltpu.PrefetchScalarGridSpec(
            num_scalar_prefetch=2,
            grid=(group, per_block),
            in_specs=[part(task) for task in range(tasks)] + [rows],
            out_specs=rows,
        ),
        name="merge",
    )(slots, live, *([received] * tasks), base)


def arrive(like, target, send_sem, recv_sem, peer):
    return pltpu.make_async_remote_copy(
        src_ref=like, dst_ref=target, send_sem=send_sem, recv_sem=recv_sem,
        device_id=peer, device_id_type=MESH,
    )


def spread_body(packed, plan, direct, gathered, plans, p_send, p_recv, d_send, d_recv, g_send, g_recv, own_sem):
    expert, task, shard = (lax.axis_index(a) for a in ("expert", "task", "shard"))
    block = expert * 4 + shard
    owner, place = block // 2, block % 2
    half, x, y = shard // 2, task % 2, task // 2
    peer = (1 - expert, task, shard)
    part = (DIRECT, (TILE - DIRECT) // 2)
    far = pl.ds(pl.multiple_of(2 * (1 - half), 2), 2)

    def straight(de, ds):
        to_expert, to_shard = (expert + de) % 2, (shard + ds) % 4
        rows = packed.at[to_expert, to_shard, :, :, pl.ds(0, DIRECT)]
        return rows, pltpu.make_async_remote_copy(
            src_ref=rows, dst_ref=direct.at[task, place],
            send_sem=d_send.at[de, ds], recv_sem=d_recv.at[task, place],
            device_id=(to_expert, owner, to_shard), device_id_type=MESH,
        )

    def partial(de, dx):
        to_expert, to_x = (expert + de) % 2, (x + dx) % 2
        start = pl.multiple_of(part[0] + part[1] * to_x, 16)
        rows = packed.at[to_expert, far, :, :, pl.ds(start, part[1])]
        return rows, pltpu.make_async_remote_copy(
            src_ref=rows, dst_ref=gathered.at[task],
            send_sem=g_send.at[de, dx], recv_sem=g_recv.at[task],
            device_id=(to_expert, 2 * expert + to_x, shard), device_id_type=MESH,
        )

    def tell(step):
        return pltpu.make_async_remote_copy(
            src_ref=plan, dst_ref=plans.at[task],
            send_sem=p_send.at[step], recv_sem=p_recv.at[task],
            device_id=(expert, (task + step) % 4, shard), device_id_type=MESH,
        )

    told = pltpu.make_async_copy(plan, plans.at[task], own_sem.at[2])
    told.start()
    for step in range(1, 4):
        tell(step).start()
    copies = []
    for de in range(2):
        for dx in (1, 0):
            own = y == expert if (de, dx) == (0, 0) else None
            copies.append((partial(de, dx), own, gathered.at[task], own_sem.at[0]))
    for ds in (2, 1, 3, 0):
        for de in range(2):
            own = owner == task if (de, ds) == (0, 0) else None
            copies.append((straight(de, ds), own, direct.at[task, place], own_sem.at[1]))
    for (rows, copy), own, target, sem in copies:
        if own is None:
            copy.start()
        else:
            pl.when(own)(pltpu.make_async_copy(rows, target, sem).start)
            pl.when(jnp.logical_not(own))(copy.start)
    for source in range(4):
        come = arrive(plans.at[source], plans.at[source], p_send.at[0], p_recv.at[source], peer)
        pl.when(task != source)(come.wait_recv)
        local = jnp.logical_and(y == expert, task == source)
        come = arrive(gathered.at[source], gathered.at[source], g_send.at[0, 0], g_recv.at[source], peer)
        pl.when(jnp.logical_not(local))(come.wait_recv)
        for at in range(2):
            local = jnp.logical_and(owner == task, jnp.logical_and(task == source, place == at))
            come = arrive(direct.at[source, at], direct.at[source, at], d_send.at[0, 0], d_recv.at[source, at], peer)
            pl.when(jnp.logical_not(local))(come.wait_recv)
    told.wait()
    for step in range(1, 4):
        tell(step).wait_send()
    for (rows, copy), own, target, sem in copies:
        if own is None:
            copy.wait_send()
        else:
            pl.when(own)(pltpu.make_async_copy(rows, target, sem).wait)
            pl.when(jnp.logical_not(own))(copy.wait_send)


def spread(packed, plan):
    _, _, _, cap, _, width = packed.shape
    return pl.pallas_call(
        spread_body,
        out_shape=(
            jax.ShapeDtypeStruct((4, 2, 2, cap, DIRECT, width), packed.dtype),
            jax.ShapeDtypeStruct((4, 2, 2, cap, (TILE - DIRECT) // 2, width), packed.dtype),
            jax.ShapeDtypeStruct((4,) + plan.shape, plan.dtype),
        ),
        in_specs=[pl.BlockSpec(memory_space=pl.ANY)] * 2,
        out_specs=(pl.BlockSpec(memory_space=pl.ANY),) * 3,
        scratch_shapes=[
            pltpu.SemaphoreType.DMA((4,)),
            pltpu.SemaphoreType.DMA((4,)),
            pltpu.SemaphoreType.DMA((2, 4)),
            pltpu.SemaphoreType.DMA((4, 2)),
            pltpu.SemaphoreType.DMA((2, 2)),
            pltpu.SemaphoreType.DMA((4,)),
            pltpu.SemaphoreType.DMA((3,)),
        ],
        compiler_params=pltpu.CompilerParams(has_side_effects=True),
        name="spread",
    )(packed, plan)


def deliver_body(packed, sums, near, far, n_send, n_recv, f_send, f_recv, own_sem):
    expert, task, shard = (lax.axis_index(a) for a in ("expert", "task", "shard"))
    block = expert * 4 + shard
    owner, place = block // 2, block % 2
    half, x, y = shard // 2, task % 2, task // 2
    peer = (1 - expert, task, shard)
    rest = pl.ds(DIRECT, TILE - DIRECT)
    is_near = x == half

    def reduced(i):
        return pltpu.make_async_remote_copy(
            src_ref=sums.at[i], dst_ref=far.at[shard % 2, x],
            send_sem=f_send.at[i], recv_sem=f_recv.at[shard % 2, x],
            device_id=(expert, 2 * y + half, 2 * (1 - half) + i), device_id_type=MESH,
        )

    def straight(de, di):
        to_expert = (expert + de) % 2
        to_shard = 2 * half + (shard + di) % 2
        rows = packed.at[to_expert, to_shard, :, :, rest]
        return rows, pltpu.make_async_remote_copy(
            src_ref=rows, dst_ref=near.at[task, place],
            send_sem=n_send.at[de, di], recv_sem=n_recv.at[task, place],
            device_id=(to_expert, owner, to_shard), device_id_type=MESH,
        )

    for i in range(2):
        reduced(i).start()
    own = owner == task
    for de, di in ((0, 1), (1, 1), (1, 0)):
        straight(de, di)[1].start()
    rows, copy = straight(0, 0)
    kept = pltpu.make_async_copy(rows, near.at[task, place], own_sem)
    pl.when(own)(kept.start)
    pl.when(jnp.logical_not(own))(copy.start)

    for at in range(2):
        for source in range(2):
            come = arrive(far.at[at, source], far.at[at, source], f_send.at[0], f_recv.at[at, source], peer)
            pl.when(jnp.logical_not(is_near))(come.wait_recv)
        for source in range(4):
            local = jnp.logical_and(own, jnp.logical_and(task == source, place == at))
            come = arrive(near.at[source, at], near.at[source, at], n_send.at[0, 0], n_recv.at[source, at], peer)
            pl.when(jnp.logical_and(is_near, jnp.logical_not(local)))(come.wait_recv)
    for i in range(2):
        reduced(i).wait_send()
    for de, di in ((0, 1), (1, 1), (1, 0)):
        straight(de, di)[1].wait_send()
    pl.when(own)(kept.wait)
    pl.when(jnp.logical_not(own))(copy.wait_send)


def deliver(packed, sums):
    _, _, _, cap, _, width = packed.shape
    return pl.pallas_call(
        deliver_body,
        out_shape=(
            jax.ShapeDtypeStruct((4, 2, 2, cap, TILE - DIRECT, width), packed.dtype),
            jax.ShapeDtypeStruct((2, 2) + sums.shape[1:], packed.dtype),
        ),
        in_specs=[pl.BlockSpec(memory_space=pl.ANY)] * 2,
        out_specs=(pl.BlockSpec(memory_space=pl.ANY),) * 2,
        scratch_shapes=[
            pltpu.SemaphoreType.DMA((2, 2)),
            pltpu.SemaphoreType.DMA((4, 2)),
            pltpu.SemaphoreType.DMA((2,)),
            pltpu.SemaphoreType.DMA((2, 2)),
            pltpu.SemaphoreType.DMA,
        ],
        compiler_params=pltpu.CompilerParams(has_side_effects=True),
        name="deliver",
    )(packed, sums)


def reduce_body(slots, live, *refs):
    parts, sums = refs[:4], refs[4]
    tile = pl.program_id(0)
    total = jnp.zeros(sums.shape[:2] + sums.shape[3:], jnp.float32)
    for task, part in enumerate(parts):
        kept = live[task * pl.num_programs(0) + tile].astype(jnp.float32)
        total += part[0, :, :, 0].astype(jnp.float32) * kept
    sums[:, :, 0] = total.astype(jnp.bfloat16)


def reduce(slots, live, gathered):
    rows, width = gathered.shape[-2:]
    per_block = slots.shape[0] // 4

    def part(task):
        return pl.BlockSpec(
            (1, 2, 2, 1, rows, width),
            lambda j, slots, live: (task, 0, 0, slots[task * per_block + j], 0, 0),
        )

    return pl.pallas_call(
        reduce_body,
        out_shape=jax.ShapeDtypeStruct((2, 2, per_block, rows, width), jnp.bfloat16),
        grid_spec=pltpu.PrefetchScalarGridSpec(
            num_scalar_prefetch=2,
            grid=(per_block,),
            in_specs=[part(task) for task in range(4)],
            out_specs=pl.BlockSpec((2, 2, 1, rows, width), lambda j, slots, live: (0, 0, j, 0, 0)),
        ),
        name="reduce",
    )(slots, live, *([gathered] * 4))


def finish_body(slots, live, near_flag, *refs):
    direct, near, far, base, merged = refs[:4], refs[4:8], refs[8], refs[9], refs[10]
    at = pl.program_id(0) * pl.num_programs(1) + pl.program_id(1)
    count = pl.num_programs(0) * pl.num_programs(1)
    kept = [live[task * count + at].astype(jnp.float32) for task in range(4)]

    def settle(rows, numerator, denominator):
        numerator += PRIOR_WEIGHT * base[rows].astype(jnp.float32)
        merged[rows] = (numerator / (denominator + PRIOR_WEIGHT)).astype(jnp.bfloat16)

    def added(parts, which):
        return sum(p[0, 0, which, 0].astype(jnp.float32) * k for p, k in zip(parts, kept))

    settle(pl.ds(0, DIRECT), added(direct, 0), added(direct, 1))

    @pl.when(near_flag[0] == 1)
    def _():
        settle(pl.ds(DIRECT, TILE - DIRECT), added(near, 0), added(near, 1))

    @pl.when(near_flag[0] == 0)
    def _():
        size = (TILE - DIRECT) // 2
        for x in range(2):
            settle(
                pl.ds(DIRECT + size * x, size),
                far[0, x, 0, 0].astype(jnp.float32),
                far[0, x, 1, 0].astype(jnp.float32),
            )


def finish(slots, live, near_flag, direct, near, far, base):
    width = base.shape[-1]
    per_block = slots.shape[0] // 8

    def direct_part(task):
        return pl.BlockSpec(
            (1, 1, 2, 1, DIRECT, width),
            lambda g, j, slots, live, flag: (task, g, 0, slots[(task * 2 + g) * per_block + j], 0, 0),
        )

    def near_part(task):
        return pl.BlockSpec(
            (1, 1, 2, 1, TILE - DIRECT, width),
            lambda g, j, slots, live, flag: (
                task, g * flag[0], 0, slots[(task * 2 + g) * per_block + j] * flag[0], 0, 0
            ),
        )

    far_part = pl.BlockSpec(
        (1, 2, 2, 1, (TILE - DIRECT) // 2, width),
        lambda g, j, slots, live, flag: (g * (1 - flag[0]), 0, 0, j * (1 - flag[0]), 0, 0),
    )
    rows = pl.BlockSpec((TILE, width), lambda g, j, slots, live, flag: (g * per_block + j, 0))
    return pl.pallas_call(
        finish_body,
        out_shape=jax.ShapeDtypeStruct(base.shape, jnp.bfloat16),
        grid_spec=pltpu.PrefetchScalarGridSpec(
            num_scalar_prefetch=3,
            grid=(2, per_block),
            in_specs=[direct_part(t) for t in range(4)] + [near_part(t) for t in range(4)] + [far_part, rows],
            out_specs=rows,
        ),
        name="finish",
    )(slots, live, near_flag, *([direct] * 4), *([near] * 4), far, base)


def local(weights, fisher, base_weights, tile_list, tile_count):
    experts, tasks, shards = (lax.axis_size(a) for a in ("expert", "task", "shard"))
    expert, task, shard = (lax.axis_index(a) for a in ("expert", "task", "shard"))
    per_block = weights.shape[2] // TILE
    cap = tile_list.shape[-1]
    group = experts * shards // tasks
    block = expert * shards + shard
    slot_number = jnp.arange(cap, dtype=jnp.int32)

    own_list = lax.dynamic_index_in_dim(tile_list[0], block, 1, keepdims=False)
    own_count = lax.dynamic_index_in_dim(tile_count[0], block, 1, keepdims=False)
    own_live = (slot_number[None, :] < own_count[:, None]).astype(jnp.int32)
    packed = pack(own_list.reshape(-1), own_live.reshape(-1), weights[0], fisher[0], shards)

    marked = jnp.where(slot_number < tile_count[..., None], tile_list, per_block)
    mine = lax.dynamic_index_in_dim(marked[0], expert, 0, keepdims=False)
    small = (experts, tasks, shards) == (2, 4, 4)
    if small:
        plan = jnp.pad(mine, ((0, 0), (0, 128 - cap)))
        direct, gathered, plans = spread(packed, plan)
        plans = plans[:, :, :cap]
    else:
        plans = lax.all_gather(marked[0], "task")
        plans = lax.dynamic_index_in_dim(plans, expert, 1, keepdims=False)

    def lookup(start, count):
        part = lax.dynamic_slice_in_dim(plans, start, count, 1)
        hits = part[..., None] == jnp.arange(per_block, dtype=jnp.int32)
        slots = jnp.sum(hits * slot_number[:, None], axis=2).astype(jnp.int32)
        return slots.reshape(-1), jnp.any(hits, axis=2).astype(jnp.int32).reshape(-1)

    slots, live = lookup(task * group, group)
    if small:
        sums = reduce(*lookup((task // 2) * shards + shard, 1), gathered)
        near, far = deliver(packed, sums)
        flag = (task % 2 == shard // 2).astype(jnp.int32).reshape(1)
        return finish(slots, live, flag, direct, near, far, base_weights[0])[None]
    received = exchange(packed, (experts, tasks, shards))
    return merge(slots, live, received, base_weights[0])[None]


def solution(mesh):
    in_specs = (
        P("task", None, ("expert", "shard"), None),
        P("task", None, ("expert", "shard"), None),
        P("expert", "task", "shard"),
        P("task", None, None, None),
        P("task", None, None),
    )
    out_specs = P("expert", "task", "shard")
    return jax.shard_map(local, mesh=mesh, in_specs=in_specs, out_specs=out_specs, check_vma=False)
```
